32 devices in a mesh: groups: 2 (over y), ep: 8 (over z, core), tp: 2 (over x).
Axes of the slice: x: 2, y: 2, z: 4, core: 2. Of those that a mesh axis runs over, the one named last changes fastest.
Arguments:
- hidden: bfloat16 [1024, 2880], P(('groups', 'ep')), parts along dimension 0, may hold values from -6 to 6
- route_experts: int32 [1024, 4], P(('groups', 'ep')), parts along dimension 0, may hold values from 0 to 7, all different within a row; in each aligned block of 64 rows (0 to 63, 64 to 127, ...) at most 64 rows name the same one
- route_weight: float32 [1024, 4], P(('groups', 'ep')), parts along dimension 0, may hold values from 0.1 to 0.6
- norm_gain: bfloat16 [2880], replicated, may hold values from 0.099609375 to 1.8984375
- gate_up_codes: int32 [8, 360, 5120], P('ep', None, 'tp'), may hold values from -2147483648 to 2147483646
- gate_up_scales: bfloat16 [8, 90, 5120], P('ep', None, 'tp'), as said below
- gate_up_bias: bfloat16 [8, 5120], P('ep', 'tp'), may hold values from -3 to 3
- down_codes: int32 [8, 2560, 360], P('ep', 'tp'), may hold values from -2147483648 to 2147483646
- down_scales: bfloat16 [8, 80, 2880], P('ep', 'tp'), as said below
- down_bias: bfloat16 [8, 2880], P('ep', 'tp'), may hold values from -3 to 3
Outputs:
- layer_out: bfloat16 [1024, 2880], P(('groups', 'ep'), 'tp'), parts along dimension 0
The draws below stay inside these ranges and needn't reach their ends.
There are 2 independent parts, one for each index of `groups`. The reference program is written for one: setup_inputs(seed, part) draws one part's arguments, and reference() takes and returns one part's arrays. A program takes and returns all parts, laid end to end along the dimension named above; an argument that names none is the same for every part. Nothing has to cross between parts.
Inputs may be any that keep to these rules, and one draw needn't show every extreme that they name: `route_experts`: each row names 4 different experts. In each aligned block of 64 rows no expert is named by more than 64 rows, and in some blocks one expert is named by exactly 64 rows. `gate_up_scales`: every scale is a power of two. `down_scales`: every scale is a power of two.
All inputs are finite; a program needn't handle non-finite values.
Results may differ from the reference program's by a relative error of at most 0.013.
Values may be sent and summed in bfloat16 or wider, within the bound.
No kernel may reach another device: no remote copies, remote signals or barrier semaphores. Data moves between devices by JAX's collectives and lax.ppermute only.
A program may use at most 128 MiB of HBM per device.

```python
import math
import jax
import jax.numpy as jnp
import numpy as np
from jax import lax

D = 2880
TOP = 4
FF = 2560
TOK_EP = 64
EXPERTS = 8
TOKENS = 512
CAP = 64
N_EP = 8
N_TP = 2


def draw_gate_up_scales(key, part):
    centre = int(math.floor(math.log2(0.5 / math.sqrt(D))))
    powers = jax.random.randint(jax.random.fold_in(key, 11), (EXPERTS, D // 32, 2 * FF), centre - 1, centre + 2)
    return jnp.exp2(powers.astype(jnp.float32)).astype(jnp.bfloat16)


def draw_down_scales(key, part):
    centre = int(math.floor(math.log2(0.5 / math.sqrt(FF))))
    powers = jax.random.randint(jax.random.fold_in(key, 23), (EXPERTS, FF // 32, D), centre - 1, centre + 2)
    return jnp.exp2(powers.astype(jnp.float32)).astype(jnp.bfloat16)


def place_ends(entries, stream_key, smallest, largest):
    extent = entries.shape
    index_at = [jax.random.randint(jax.random.fold_in(stream_key, axis), (), 0, extent[axis]) for axis in range(len(extent))]
    entries = entries.at[tuple(index_at)].set(smallest)
    longest = extent.index(max(extent))
    index_at[longest] = (index_at[longest] + 1) % extent[longest]
    return entries.at[tuple(index_at)].set(largest)


def shard_levels(own_key, extent, cuts, low, high):
    def one(axis_at, blocks):
        heights = jax.random.uniform(jax.random.fold_in(jax.random.fold_in(own_key, 6), axis_at), (blocks,), jnp.float32, low / len(cuts), high / len(cuts))
        return jnp.repeat(jnp.exp(heights), extent[axis_at] // blocks).reshape((-1,) + (1,) * (len(extent) - axis_at - 1))

    level = one(*cuts[0])
    for cut in cuts[1:]:
        level = level * one(*cut)
    return level


def shared_out(rng, own, number, rows, amount, top, reach, slope):
    ranking = jax.random.permutation(rng, amount)
    crowded, common = load_shares(amount, rows * top, reach, slope, True), load_shares(amount, rows * top, reach, slope, False)
    places = jnp.arange(amount)

    def named(lengths, offset_by):
        used = int((lengths > 0).sum())
        fixed = max(1, used // 4)
        moved = fixed + (places - fixed + offset_by * (used - fixed)) % max(1, amount - fixed)
        return jnp.zeros((amount,), jnp.int32).at[ranking[jnp.where(places < fixed, places, moved)]].set(jnp.asarray(lengths, jnp.int32))

    lengths = jnp.where(number % 4 == 0, named(crowded, number // 4), named(common, number - number // 4 - 1))
    mixed = jax.random.permutation(jax.random.fold_in(own, 3), amount)
    giver, taker = mixed[0:amount // 2 * 2:2], mixed[1:amount // 2 * 2:2]
    margin = jnp.minimum(lengths[giver] - 1, reach - lengths[taker]) // 2
    margin = jnp.where((giver == ranking[0]) | (taker == ranking[0]) | (lengths[taker] == 0), 0, jnp.maximum(margin, 0))
    moved = jax.random.randint(jax.random.fold_in(own, 4), (amount // 2,), 0, 1 << 20) % (margin + 1)
    lengths = lengths.at[giver].add(-moved).at[taker].add(moved)
    items = jnp.searchsorted(jnp.cumsum(lengths), jnp.arange(rows * top), side="right").astype(jnp.int32)
    grid = items.reshape(top, rows).T
    grid = grid[jax.random.permutation(jax.random.fold_in(own, 1), rows)]
    offset_by = jax.random.randint(jax.random.fold_in(own, 2), (rows, 1), 0, top)
    return jnp.take_along_axis(grid, (jnp.arange(top)[None, :] + offset_by) % top, axis=1)


def load_shares(number_of, total, reach, skew, full):
    portions = [(1 << 20) // math.isqrt(standing ** skew) + 1 for standing in range(1, number_of + 1)]
    largest = reach if full else min(reach, max(-(-total // number_of), total * portions[0] // sum(portions)))
    least = 1 if total - largest >= number_of - 1 else 0
    holding, surplus = [largest] + [least] * (number_of - 1), total - largest - least * (number_of - 1)
    while surplus > 0:
        free = [i for i in range(1, number_of) if holding[i] < largest] or [i for i in range(1, number_of) if holding[i] < reach]
        whole, budget = sum([portions[i] for i in free]), surplus
        for i in free:
            extra = min(reach - holding[i], max(1, budget * portions[i] // whole), surplus)
            holding[i] = holding[i] + extra
            surplus = surplus - extra
    return np.array(holding)


def bell_draw(rng, extent, spread, reach, shards=(), held_as=jnp.bfloat16):
    gain = shard_levels(rng, extent, shards, -0.22, 0.18) if shards else 1.0
    entries = jax.random.normal(rng, extent, jnp.float32) * spread * gain
    return jnp.minimum(jnp.maximum(entries, -reach), reach).astype(held_as)


def setup_inputs(seed: int = 0, part: int = 0) -> dict:
    key_of = jax.random.split(jax.random.key(seed), 11)
    part_splits = jax.random.split(jax.random.fold_in(key_of[10], part), 11)
    hidden = bell_draw(part_splits[0], (TOKENS, D), 1.0, 6.0, ((0, 8),))
    route_experts_keys = jax.random.split(jax.random.fold_in(part_splits[1], 1), TOKENS // TOK_EP)
    route_experts_turns = jax.random.permutation(jax.random.fold_in(part_splits[1], 3), TOKENS // TOK_EP)
    route_experts = jax.vmap(lambda own, number: shared_out(jax.random.fold_in(part_splits[1], 2), own, number, TOK_EP, EXPERTS, TOP, CAP, 2))(route_experts_keys, route_experts_turns).reshape((TOKENS, TOP))
    route_weight = jnp.clip(0.1 + 0.5 * jax.random.uniform(part_splits[2], (TOKENS, TOP), jnp.float32) ** shard_levels(part_splits[2], (TOKENS, TOP), ((0, 8),), -0.2, 0.2), 0.1, 0.6)
    norm_gain = jnp.clip(1.0 + 0.18 * jax.random.normal(key_of[3], (D,), jnp.float32), 0.099609375, 1.8984375).astype(jnp.bfloat16)
    gate_up_codes = place_ends(jax.random.randint(key_of[4], (EXPERTS, D // 8, 2 * FF), -2147483648, 2147483647), jax.random.fold_in(key_of[4], 1), -2147483648, 2147483646).astype(jnp.int32)
    gate_up_scales = draw_gate_up_scales(jax.random.fold_in(key_of[10], 71), part)
    gate_up_bias = bell_draw(key_of[6], (EXPERTS, 2 * FF), 0.5, 3.0, ((0, 8), (1, 2)))
    down_codes = place_ends(jax.random.randint(key_of[7], (EXPERTS, FF, D // 8), -2147483648, 2147483647), jax.random.fold_in(key_of[7], 1), -2147483648, 2147483646).astype(jnp.int32)
    down_scales = draw_down_scales(jax.random.fold_in(key_of[10], 71), part)
    down_bias = bell_draw(key_of[9], (EXPERTS, D), 0.5, 3.0, ((0, 8), (1, 2)))
    return {"hidden": hidden, "route_experts": route_experts, "route_weight": route_weight, "norm_gain": norm_gain, "gate_up_codes": gate_up_codes, "gate_up_scales": gate_up_scales, "gate_up_bias": gate_up_bias, "down_codes": down_codes, "down_scales": down_scales, "down_bias": down_bias}


def decode_nibble(nibble):
    magnit = nibble & 7
    exponent = jnp.maximum(jnp.right_shift(magnit, 1) - 1, 0)
    doubled = jnp.where(magnit < 2, magnit, jnp.left_shift(2 + (magnit & 1), exponent))
    signed_val = doubled.astype(jnp.float32) * 0.5
    return jnp.where(nibble >= 8, -signed_val, signed_val)

def unpack_weights(packed, scaling):
    row_count = packed.shape[0]
    shifts = jnp.arange(8, dtype=jnp.int32) * 4
    nibble = jnp.right_shift(packed[:, :, None], shifts[None, None, :]) & 15
    nibble = nibble.reshape(row_count, packed.shape[1] * 8)
    signed_val = decode_nibble(nibble)
    signed_val = signed_val.reshape(row_count // 32, 32, -1) * scaling.astype(jnp.float32)[:, None, :]
    return signed_val.reshape(row_count, -1).astype(jnp.bfloat16)

def unpack_rows(packed, scaling):
    row_count = packed.shape[0] * 8
    shifts = jnp.arange(8, dtype=jnp.int32) * 4
    nibble = jnp.right_shift(packed[:, None, :], shifts[None, :, None]) & 15
    nibble = nibble.reshape(row_count, packed.shape[1])
    signed_val = decode_nibble(nibble)
    signed_val = signed_val.reshape(row_count // 32, 32, -1) * scaling.astype(jnp.float32)[:, None, :]
    return signed_val.reshape(row_count, -1).astype(jnp.bfloat16)

def rms_normed(hidden, norm_gain):
    widened = hidden.astype(jnp.float32)
    mean_square = lax.optimization_barrier(jnp.mean(widened * widened, axis=-1, keepdims=True))
    scaled = widened * lax.rsqrt(mean_square + 1e-05) * norm_gain.astype(jnp.float32)
    return scaled.astype(jnp.bfloat16)

def slot_numbers(routes):
    block_count, row_count, top_count = routes.shape
    flat_routes = routes.reshape(block_count, row_count * top_count)
    onehot = (flat_routes[:, :, None] == jnp.arange(EXPERTS, dtype=jnp.int32)[None, None, :]).astype(jnp.int32)
    before = jnp.cumsum(onehot, axis=1) - onehot
    slot_of = lax.optimization_barrier(jnp.sum(before * onehot, axis=2))
    return slot_of.reshape(block_count, row_count, top_count)

def expert_rows(normed_rows, gate_codes, gate_scales, gate_bias, lower_codes, lower_scales, lower_bias):
    gate_up_weight = unpack_rows(gate_codes, gate_scales)
    down_weight = unpack_weights(lower_codes, lower_scales)
    projected = jnp.dot(normed_rows, gate_up_weight, preferred_element_type=jnp.float32) + gate_bias.astype(jnp.float32)
    gate_part = jnp.minimum(projected[:, 0::2], 7.0)
    upward = jnp.clip(projected[:, 1::2], -7.0, 7.0)
    activated = (gate_part * jax.nn.sigmoid(1.702 * gate_part) * (upward + 1.0)).astype(jnp.bfloat16)
    quarter = FF // N_TP
    summed = jnp.zeros((normed_rows.shape[0], D), jnp.float32)
    for tp_part in range(N_TP):
        partial_value = jnp.dot(activated[:, tp_part * quarter:(tp_part + 1) * quarter], down_weight[tp_part * quarter:(tp_part + 1) * quarter], preferred_element_type=jnp.float32).astype(jnp.bfloat16)
        summed = summed + partial_value.astype(jnp.float32)
    return (summed + lower_bias.astype(jnp.float32)).astype(jnp.bfloat16)

def reference(hidden, route_experts, route_weight, norm_gain, gate_up_codes, gate_up_scales, gate_up_bias, down_codes, down_scales, down_bias):
    normed = rms_normed(hidden, norm_gain)
    routes = route_experts.reshape(N_EP, TOK_EP, TOP)
    slot_of = slot_numbers(routes)
    token_ids = jnp.broadcast_to(jnp.arange(TOKENS, dtype=jnp.int32).reshape(N_EP, TOK_EP, 1), routes.shape)
    block_ids = jnp.broadcast_to(jnp.arange(N_EP, dtype=jnp.int32).reshape(N_EP, 1, 1), routes.shape)
    slot_table = jnp.zeros((EXPERTS, N_EP, CAP), jnp.int32).at[routes, block_ids, slot_of].set(token_ids)

    def one_expert(expert):
        picked = normed[slot_table[expert].reshape(-1)]
        return expert_rows(picked, gate_up_codes[expert], gate_up_scales[expert], gate_up_bias[expert], down_codes[expert], down_scales[expert], down_bias[expert])
    outputs = lax.map(one_expert, jnp.arange(EXPERTS, dtype=jnp.int32)).reshape(EXPERTS, N_EP, CAP, D)
    weights = route_weight.reshape(N_EP, TOK_EP, TOP)
    running = hidden.astype(jnp.float32).reshape(N_EP, TOK_EP, D)
    for position in range(TOP):
        fetched = outputs[routes[:, :, position], block_ids[:, :, position], slot_of[:, :, position]]
        running = running + weights[:, :, position][:, :, None] * fetched.astype(jnp.float32)
    return running.reshape(TOKENS, D).astype(jnp.bfloat16)
```

```python
import jax
import jax.numpy as jnp
from jax import lax
from jax.experimental import pallas as pl
from jax.experimental.pallas import tpu as pltpu
from jax.sharding import PartitionSpec as P

VMEM_BYTES = 56 * 1024 * 1024


def largest_step(total, limit, multiple):
    best = 0
    for size in range(multiple, min(total, limit) + 1, multiple):
        if total % size == 0:
            best = size
    return best or total


def decode_words(words, scale):
    word_count, width = words.shape
    shifts = lax.broadcasted_iota(jnp.int32, (1, 8, width), 1) * 4
    nibble = (words[:, None, :] >> shifts) & 15
    half = nibble.astype(jnp.float32).reshape(word_count * 8, width).astype(jnp.bfloat16) * 0.5
    negative = half >= 4.0
    magnit = jnp.where(negative, half - 4.0, half)
    value = magnit + jnp.maximum(magnit - 2.0, 0.0) + 2.0 * jnp.maximum(magnit - 3.0, 0.0)
    return value * jnp.where(negative, -scale, scale)


def gate_up_kernel(words_ref, scale_ref, out_ref, *, step, block_words):
    width = words_ref.shape[1]
    half = width // 2
    from_col = lax.broadcasted_iota(jnp.int32, (width, width), 0)
    to_col = lax.broadcasted_iota(jnp.int32, (width, width), 1)
    wanted = jnp.where(to_col < half, 2 * to_col, 2 * (to_col - half) + 1)
    parting = (from_col == wanted).astype(jnp.bfloat16)
    blocks = step // block_words
    scales = scale_ref[...].astype(jnp.float32)
    for part in range(words_ref.shape[0] // step):
        words = words_ref[part * step : (part + 1) * step, :]
        scale = scales[part * blocks : (part + 1) * blocks, :]
        spread = jnp.broadcast_to(scale[:, None, :], (blocks, block_words * 8, width))
        spread = spread.reshape(step * 8, width).astype(jnp.bfloat16)
        value = decode_words(words, spread)
        out_ref[part * step * 8 : (part + 1) * step * 8, :] = jnp.dot(
            value, parting, preferred_element_type=jnp.float32
        ).astype(jnp.bfloat16)


def unpack_gate_up(codes, scales, tile):
    word_count, width = codes.shape
    block_words = word_count // scales.shape[0]
    step = largest_step(word_count, 80, 8)
    return pl.pallas_call(
        lambda *refs: gate_up_kernel(*refs, step=step, block_words=block_words),
        grid=(width // tile,),
        in_specs=[
            pl.BlockSpec((word_count, tile), lambda i: (0, i)),
            pl.BlockSpec((scales.shape[0], tile), lambda i: (0, i)),
        ],
        out_specs=pl.BlockSpec((word_count * 8, tile), lambda i: (0, i)),
        out_shape=jax.ShapeDtypeStruct((word_count * 8, width), jnp.bfloat16),
        compiler_params=pltpu.CompilerParams(vmem_limit_bytes=VMEM_BYTES),
        name="unpack_gate_up",
    )(codes, scales)


def down_kernel(words_ref, scale_ref, out_ref):
    unit_count = words_ref.shape[1]
    block_count = scale_ref.shape[1]
    width = unit_count // block_count
    block_of = lax.broadcasted_iota(jnp.int32, (block_count, unit_count), 1) // width
    spreading = (block_of == lax.broadcasted_iota(jnp.int32, (block_count, unit_count), 0)).astype(
        jnp.bfloat16
    )
    spread = jnp.dot(scale_ref[...], spreading, preferred_element_type=jnp.float32)
    out_ref[...] = decode_words(words_ref[...], spread.astype(jnp.bfloat16))


def unpack_down(codes, scales):
    unit_count, word_count = codes.shape
    block_count = scales.shape[0]
    step = largest_step(word_count, 40, 8)
    return pl.pallas_call(
        down_kernel,
        grid=(word_count // step,),
        in_specs=[
            pl.BlockSpec((step, unit_count), lambda i: (i, 0)),
            pl.BlockSpec((step * 8, block_count), lambda i: (i, 0)),
        ],
        out_specs=pl.BlockSpec((step * 8, unit_count), lambda i: (i, 0)),
        out_shape=jax.ShapeDtypeStruct((word_count * 8, unit_count), jnp.bfloat16),
        compiler_params=pltpu.CompilerParams(vmem_limit_bytes=VMEM_BYTES),
        name="unpack_down",
    )(codes.T, scales.T)


def hidden_kernel(rows_ref, weight_ref, bias_ref, out_ref):
    model_width, width = weight_ref.shape
    half = width // 2
    projected = jnp.dot(
        rows_ref[:, :model_width], weight_ref[...], preferred_element_type=jnp.float32
    ) + bias_ref[...]
    gate = jnp.minimum(projected[:, :half], 7.0)
    upward = jnp.clip(projected[:, half:], -7.0, 7.0)
    out_ref[...] = (gate * jax.nn.sigmoid(1.702 * gate) * (upward + 1.0)).astype(jnp.bfloat16)


def hidden_units(rows, weight, bias, tile):
    row_count = rows.shape[0]
    model_width, width = weight.shape
    return pl.pallas_call(
        hidden_kernel,
        grid=(width // tile,),
        in_specs=[
            pl.BlockSpec(rows.shape, lambda i: (0, 0)),
            pl.BlockSpec((model_width, tile), lambda i: (0, i)),
            pl.BlockSpec((1, tile), lambda i: (0, i)),
        ],
        out_specs=pl.BlockSpec((row_count, tile // 2), lambda i: (0, i)),
        out_shape=jax.ShapeDtypeStruct((row_count, width // 2), jnp.bfloat16),
        compiler_params=pltpu.CompilerParams(vmem_limit_bytes=VMEM_BYTES),
        name="hidden_units",
    )(rows, weight, bias)


def project_kernel(rows_ref, weight_ref, bias_ref, factor_ref, out_ref):
    value = lax.dot_general(
        rows_ref[...], weight_ref[...], (((1,), (1,)), ((), ())), preferred_element_type=jnp.float32
    )
    out_ref[...] = ((value + bias_ref[...]) * factor_ref[...]).astype(jnp.bfloat16)


def project_down(rows, weight, bias, factor):
    row_count, unit_count = rows.shape
    model_width = weight.shape[0]
    tile = 512
    return pl.pallas_call(
        project_kernel,
        grid=(pl.cdiv(model_width, tile),),
        in_specs=[
            pl.BlockSpec((row_count, unit_count), lambda i: (0, 0)),
            pl.BlockSpec((tile, unit_count), lambda i: (i, 0)),
            pl.BlockSpec((1, tile), lambda i: (0, i)),
            pl.BlockSpec((row_count, 1), lambda i: (0, 0)),
        ],
        out_specs=pl.BlockSpec((row_count, tile), lambda i: (0, i)),
        out_shape=jax.ShapeDtypeStruct((row_count, model_width), jnp.bfloat16),
        compiler_params=pltpu.CompilerParams(vmem_limit_bytes=VMEM_BYTES),
        name="project_down",
    )(rows, weight, bias, factor)


def rms_normed(hidden, norm_gain):
    widened = hidden.astype(jnp.float32)
    mean_square = jnp.mean(widened * widened, axis=-1, keepdims=True)
    scaled = widened * lax.rsqrt(mean_square + 1e-05) * norm_gain.astype(jnp.float32)
    return scaled.astype(jnp.bfloat16)


def parted_bias(bias, tile):
    width = bias.shape[1]
    return bias.reshape(width // tile, tile // 2, 2).swapaxes(1, 2).reshape(1, width).astype(jnp.float32)


def shards(
    hidden,
    route_experts,
    route_weight,
    norm_gain,
    gate_up_codes,
    gate_up_scales,
    gate_up_bias,
    down_codes,
    down_scales,
    down_bias,
):
    ep_count = lax.axis_size("ep")
    ep_rank = lax.axis_index("ep")
    tp_count = lax.axis_size("tp")
    tp_rank = lax.axis_index("tp")
    tok_count, model_width = hidden.shape
    top_count = route_experts.shape[1]
    quarter = model_width // tp_count
    tile = 256
    capacity = min(tok_count, max(tp_count, 2 * tok_count * top_count // ep_count))
    normed = rms_normed(hidden, norm_gain)
    gate_up_weight = unpack_gate_up(gate_up_codes[0], gate_up_scales[0], tile)
    down_weight = unpack_down(down_codes[0], down_scales[0])
    up_bias = parted_bias(gate_up_bias, tile)
    own_cols = lax.dynamic_slice_in_dim(hidden, tp_rank * quarter, quarter, 1).astype(jnp.float32)
    own_bias = down_bias.astype(jnp.float32)
    lower_bias = lax.dynamic_update_slice(
        jnp.zeros((1, model_width), jnp.float32), own_bias, (0, tp_rank * quarter)
    )

    if capacity == tok_count:
        experts = jnp.arange(ep_count, dtype=jnp.int32)
        factors = jnp.sum(
            jnp.where(route_experts[:, :, None] == experts, route_weight[:, :, None], 0.0), axis=1
        )
        upper = factors.astype(jnp.bfloat16)
        rest = factors - upper.astype(jnp.float32)
        middle = rest.astype(jnp.bfloat16)
        lowest = (rest - middle.astype(jnp.float32)).astype(jnp.bfloat16)
        outgoing = jnp.concatenate([normed, upper, middle, lowest], axis=1)
        arrived = lax.all_gather(outgoing, "ep", axis=0, tiled=True)
        tail = arrived[:, model_width:].astype(jnp.float32)
        split = tail.reshape(tail.shape[0], 3, ep_count)
        factor = jnp.sum(
            jnp.where(experts == ep_rank, split, 0.0), axis=(1, 2)
        ).reshape(-1, 1)
        activated = hidden_units(arrived, gate_up_weight, up_bias, tile)
        answered = project_down(activated, down_weight, lower_bias, factor)
        summed = lax.psum_scatter(answered, "ep", scatter_dimension=0, tiled=True)
        summed = lax.psum_scatter(summed, "tp", scatter_dimension=1, tiled=True)
        return (own_cols + summed.astype(jnp.float32)).astype(jnp.bfloat16)

    flat_routes = route_experts.reshape(-1)
    onehot = (flat_routes[:, None] == jnp.arange(ep_count, dtype=jnp.int32)[None, :]).astype(
        jnp.int32
    )
    before = jnp.cumsum(onehot, axis=0) - onehot
    slot_of = jnp.sum(before * onehot, axis=1)
    target = (flat_routes * capacity + slot_of).reshape(tok_count, top_count)
    columns = jnp.arange(ep_count * capacity, dtype=jnp.int32)
    matches = target[:, :, None] == columns[None, None, :]
    placing = jnp.any(matches, axis=1).astype(jnp.bfloat16)
    weighting = jnp.sum(jnp.where(matches, route_weight[:, :, None], 0.0), axis=1)
    outgoing = lax.dot_general(
        placing, normed, (((0,), (0,)), ((), ())), preferred_element_type=jnp.float32
    ).astype(jnp.bfloat16)
    outgoing = outgoing.reshape(ep_count, capacity, model_width)
    arrived = lax.all_to_all(outgoing, "ep", split_axis=0, concat_axis=0, tiled=True)
    flat_rows = arrived.reshape(ep_count * capacity, model_width)
    activated = hidden_units(flat_rows, gate_up_weight, up_bias, tile)
    ones = jnp.ones((ep_count * capacity, 1), jnp.float32)
    partial_value = project_down(activated, down_weight, lower_bias, ones)
    answered = lax.psum_scatter(partial_value, "tp", scatter_dimension=1, tiled=True)
    answered = answered.reshape(ep_count, capacity, quarter)
    came_back = lax.all_to_all(answered, "ep", split_axis=0, concat_axis=0, tiled=True)
    gathered = came_back.reshape(ep_count * capacity, quarter).astype(jnp.float32)
    layer_out = own_cols + jnp.dot(weighting, gathered, precision=lax.Precision.HIGHEST)
    return layer_out.astype(jnp.bfloat16)


def solution(mesh):
    placed = (
        P(("groups", "ep"), None),
        P(("groups", "ep"), None),
        P(("groups", "ep"), None),
        P(),
        P("ep", None, "tp"),
        P("ep", None, "tp"),
        P("ep", "tp"),
        P("ep", "tp", None),
        P("ep", "tp", None),
        P("ep", "tp"),
    )
    return jax.shard_map(
        shards, mesh=mesh, in_specs=placed, out_specs=P(("groups", "ep"), "tp"), check_vma=False
    )
```

```python
import jax
import jax.numpy as jnp
from jax import lax
from jax.experimental import pallas as pl
from jax.experimental.pallas import tpu as pltpu
from jax.sharding import PartitionSpec as P

VMEM_BYTES = 56 * 1024 * 1024
PIECES = 2


def largest_step(total, limit, multiple):
    best = 0
    for size in range(multiple, min(total, limit) + 1, multiple):
        if total % size == 0:
            best = size
    return best or total


def decode_words(words, scale):
    word_count, width = words.shape
    shifts = lax.broadcasted_iota(jnp.int32, (1, 8, width), 1) * 4
    nibble = (words[:, None, :] >> shifts) & 15
    half = nibble.astype(jnp.float32).reshape(word_count * 8, width).astype(jnp.bfloat16) * 0.5
    negative = half >= 4.0
    magnit = jnp.where(negative, half - 4.0, half)
    value = magnit + jnp.maximum(magnit - 2.0, 0.0) + 2.0 * jnp.maximum(magnit - 3.0, 0.0)
    return value * jnp.where(negative, -scale, scale)


def gate_up_kernel(words_ref, scale_ref, bias_ref, out_ref, bias_out_ref, *, step, block_words):
    width = words_ref.shape[1]
    half = width // 2
    from_col = lax.broadcasted_iota(jnp.int32, (width, width), 0)
    to_col = lax.broadcasted_iota(jnp.int32, (width, width), 1)
    wanted = jnp.where(to_col < half, 2 * to_col, 2 * (to_col - half) + 1)
    parting = (from_col == wanted).astype(jnp.bfloat16)
    bias_out_ref[...] = jnp.dot(bias_ref[...], parting, preferred_element_type=jnp.float32)
    blocks = step // block_words
    scales = scale_ref[...].astype(jnp.float32)
    for part in range(words_ref.shape[0] // step):
        words = words_ref[part * step : (part + 1) * step, :]
        scale = scales[part * blocks : (part + 1) * blocks, :]
        spread = jnp.broadcast_to(scale[:, None, :], (blocks, block_words * 8, width))
        spread = spread.reshape(step * 8, width).astype(jnp.bfloat16)
        value = decode_words(words, spread)
        out_ref[part * step * 8 : (part + 1) * step * 8, :] = jnp.dot(
            value, parting, preferred_element_type=jnp.float32
        ).astype(jnp.bfloat16)


def unpack_gate_up(codes, scales, bias, tile):
    word_count, width = codes.shape
    block_words = word_count // scales.shape[0]
    step = largest_step(word_count, 80, 8)
    return pl.pallas_call(
        lambda *refs: gate_up_kernel(*refs, step=step, block_words=block_words),
        grid=(width // tile,),
        in_specs=[
            pl.BlockSpec((word_count, tile), lambda i: (0, i)),
            pl.BlockSpec((scales.shape[0], tile), lambda i: (0, i)),
            pl.BlockSpec((1, tile), lambda i: (0, i)),
        ],
        out_specs=[
            pl.BlockSpec((word_count * 8, tile), lambda i: (0, i)),
            pl.BlockSpec((1, tile), lambda i: (0, i)),
        ],
        out_shape=[
            jax.ShapeDtypeStruct((word_count * 8, width), jnp.bfloat16),
            jax.ShapeDtypeStruct((1, width), jnp.float32),
        ],
        compiler_params=pltpu.CompilerParams(vmem_limit_bytes=VMEM_BYTES),
        name="unpack_gate_up",
    )(codes, scales, bias)


def down_kernel(words_ref, scale_ref, out_ref):
    unit_count = words_ref.shape[1]
    block_count = scale_ref.shape[1]
    width = unit_count // block_count
    block_of = lax.broadcasted_iota(jnp.int32, (block_count, unit_count), 1) // width
    spreading = (block_of == lax.broadcasted_iota(jnp.int32, (block_count, unit_count), 0)).astype(
        jnp.bfloat16
    )
    spread = jnp.dot(scale_ref[...], spreading, preferred_element_type=jnp.float32)
    out_ref[...] = decode_words(words_ref[...], spread.astype(jnp.bfloat16))


def unpack_down(codes, scales):
    unit_count, word_count = codes.shape
    block_count = scales.shape[0]
    step = largest_step(word_count, 40, 8)
    return pl.pallas_call(
        down_kernel,
        grid=(word_count // step,),
        in_specs=[
            pl.BlockSpec((step, unit_count), lambda i: (i, 0)),
            pl.BlockSpec((step * 8, block_count), lambda i: (i, 0)),
        ],
        out_specs=pl.BlockSpec((step * 8, unit_count), lambda i: (i, 0)),
        out_shape=jax.ShapeDtypeStruct((word_count * 8, unit_count), jnp.bfloat16),
        compiler_params=pltpu.CompilerParams(vmem_limit_bytes=VMEM_BYTES),
        name="unpack_down",
    )(codes.T, scales.T)


def hidden_kernel(rows_ref, weight_ref, bias_ref, out_ref):
    model_width, width = weight_ref.shape
    half = width // 2
    projected = jnp.dot(
        rows_ref[:, :model_width], weight_ref[...], preferred_element_type=jnp.float32
    ) + bias_ref[...]
    gate = jnp.minimum(projected[:, :half], 7.0)
    upward = jnp.clip(projected[:, half:], -7.0, 7.0)
    out_ref[...] = (gate * jax.nn.sigmoid(1.702 * gate) * (upward + 1.0)).astype(jnp.bfloat16)


def hidden_units(rows, weight, bias, tile):
    row_count = rows.shape[0]
    model_width, width = weight.shape
    return pl.pallas_call(
        hidden_kernel,
        grid=(width // tile,),
        in_specs=[
            pl.BlockSpec(rows.shape, lambda i: (0, 0)),
            pl.BlockSpec((model_width, tile), lambda i: (0, i)),
            pl.BlockSpec((1, tile), lambda i: (0, i)),
        ],
        out_specs=pl.BlockSpec((row_count, tile // 2), lambda i: (0, i)),
        out_shape=jax.ShapeDtypeStruct((row_count, width // 2), jnp.bfloat16),
        compiler_params=pltpu.CompilerParams(vmem_limit_bytes=VMEM_BYTES),
        name="hidden_units",
    )(rows, weight, bias)


def project_kernel(rows_ref, weight_ref, bias_ref, tail_ref, pick_ref, out_ref):
    value = lax.dot_general(
        rows_ref[...], weight_ref[...], (((1,), (1,)), ((), ())), preferred_element_type=jnp.float32
    )
    factor = jnp.sum(tail_ref[...].astype(jnp.float32) * pick_ref[...], axis=1, keepdims=True)
    out_ref[...] = ((value + bias_ref[...]) * factor).astype(jnp.bfloat16)


def project_down(rows, weight, bias, tail, pick):
    row_count, unit_count = rows.shape
    model_width = weight.shape[0]
    tile = 512
    return pl.pallas_call(
        project_kernel,
        grid=(pl.cdiv(model_width, tile),),
        in_specs=[
            pl.BlockSpec((row_count, unit_count), lambda i: (0, 0)),
            pl.BlockSpec((tile, unit_count), lambda i: (i, 0)),
            pl.BlockSpec((1, tile), lambda i: (0, i)),
            pl.BlockSpec((row_count, 128), lambda i: (0, tail.shape[1] // 128 - 1)),
            pl.BlockSpec((1, 128), lambda i: (0, 0)),
        ],
        out_specs=pl.BlockSpec((row_count, tile), lambda i: (0, i)),
        out_shape=jax.ShapeDtypeStruct((row_count, model_width), jnp.bfloat16),
        compiler_params=pltpu.CompilerParams(vmem_limit_bytes=VMEM_BYTES),
        name="project_down",
    )(rows, weight, bias, tail, pick)


def norm_kernel(hidden_ref, gain_ref, experts_ref, weight_ref, *out_refs, ep_count):
    tok_count, model_width = hidden_ref.shape
    total = out_refs[0].shape[1]
    widened = hidden_ref[...].astype(jnp.float32)
    mean_square = jnp.mean(widened * widened, axis=-1, keepdims=True)
    normed = (widened * lax.rsqrt(mean_square + 1e-05) * gain_ref[...].astype(jnp.float32)).astype(
        jnp.bfloat16
    )
    tail = total - model_width
    place = lax.broadcasted_iota(jnp.int32, (tok_count, tail), 1) - (tail - 3 * ep_count)
    factor = jnp.zeros((tok_count, tail), jnp.float32)
    for position in range(experts_ref.shape[1]):
        chosen = experts_ref[:, position : position + 1]
        named = (place == chosen) | (place == chosen + ep_count) | (place == chosen + 2 * ep_count)
        factor = factor + jnp.where(named, weight_ref[:, position : position + 1], 0.0)
    upper = factor.astype(jnp.bfloat16).astype(jnp.float32)
    rest = factor - upper
    middle = rest.astype(jnp.bfloat16).astype(jnp.float32)
    pieces = jnp.where(place < ep_count, upper, jnp.where(place < 2 * ep_count, middle, rest - middle))
    pieces = pieces.astype(jnp.bfloat16)
    step = tok_count // len(out_refs)
    for i, out_ref in enumerate(out_refs):
        out_ref[:, :model_width] = normed[i * step : (i + 1) * step]
        out_ref[:, model_width:] = pieces[i * step : (i + 1) * step]


def normed_with_factors(hidden, gain, route_experts, route_weight, ep_count, pieces):
    tok_count, model_width = hidden.shape
    total = -(-(model_width + 3 * ep_count) // 128) * 128
    shape = jax.ShapeDtypeStruct((tok_count // pieces, total), jnp.bfloat16)
    return pl.pallas_call(
        lambda *refs: norm_kernel(*refs, ep_count=ep_count),
        out_shape=[shape] * pieces,
        compiler_params=pltpu.CompilerParams(vmem_limit_bytes=VMEM_BYTES),
        name="norm",
    )(hidden, gain.reshape(1, -1), route_experts, route_weight)


def rms_normed(hidden, norm_gain):
    widened = hidden.astype(jnp.float32)
    mean_square = jnp.mean(widened * widened, axis=-1, keepdims=True)
    scaled = widened * lax.rsqrt(mean_square + 1e-05) * norm_gain.astype(jnp.float32)
    return scaled.astype(jnp.bfloat16)


def tp_sum(rows, tp_rank, tp_count, quarter):
    summed = lax.dynamic_slice_in_dim(rows, tp_rank * quarter, quarter, 1).astype(jnp.float32)
    for away in range(1, tp_count):
        other = (tp_rank + away) % tp_count
        sent = lax.dynamic_slice_in_dim(rows, other * quarter, quarter, 1)
        got = lax.ppermute(sent, "tp", [(k, (k + away) % tp_count) for k in range(tp_count)])
        summed = summed + got.astype(jnp.float32)
    return summed


def shards(
    hidden,
    route_experts,
    route_weight,
    norm_gain,
    gate_up_codes,
    gate_up_scales,
    gate_up_bias,
    down_codes,
    down_scales,
    down_bias,
):
    ep_count = lax.axis_size("ep")
    ep_rank = lax.axis_index("ep")
    tp_count = lax.axis_size("tp")
    tp_rank = lax.axis_index("tp")
    tok_count, model_width = hidden.shape
    top_count = route_experts.shape[1]
    quarter = model_width // tp_count
    tile = 256
    capacity = min(tok_count, max(tp_count, 2 * tok_count * top_count // ep_count))
    gate_up_weight, up_bias = unpack_gate_up(
        gate_up_codes[0], gate_up_scales[0], gate_up_bias, tile
    )
    down_weight = unpack_down(down_codes[0], down_scales[0])
    own_cols = lax.dynamic_slice_in_dim(hidden, tp_rank * quarter, quarter, 1).astype(jnp.float32)
    own_bias = down_bias.astype(jnp.float32)
    lower_bias = lax.dynamic_update_slice(
        jnp.zeros((1, model_width), jnp.float32), own_bias, (0, tp_rank * quarter)
    )

    if capacity == tok_count and 3 * ep_count <= 128:
        place = jnp.arange(128, dtype=jnp.int32) - (128 - 3 * ep_count)
        pick = ((place >= 0) & (place % ep_count == ep_rank)).astype(jnp.float32).reshape(1, 128)
        outgoing = normed_with_factors(
            hidden, norm_gain, route_experts, route_weight, ep_count, PIECES
        )
        arrived = [lax.all_gather(rows, "ep", axis=0, tiled=True) for rows in outgoing]
        outputs = []
        for rows in arrived:
            activated = hidden_units(rows, gate_up_weight, up_bias, tile)
            answered = project_down(activated, down_weight, lower_bias, rows, pick)
            summed = lax.psum_scatter(answered, "ep", scatter_dimension=0, tiled=True)
            outputs.append(tp_sum(summed, tp_rank, tp_count, quarter))
        summed = jnp.concatenate(outputs, axis=0)
        return (own_cols + summed).astype(jnp.bfloat16)

    normed = rms_normed(hidden, norm_gain)
    flat_routes = route_experts.reshape(-1)
    onehot = (flat_routes[:, None] == jnp.arange(ep_count, dtype=jnp.int32)[None, :]).astype(
        jnp.int32
    )
    before = jnp.cumsum(onehot, axis=0) - onehot
    slot_of = jnp.sum(before * onehot, axis=1)
    target = (flat_routes * capacity + slot_of).reshape(tok_count, top_count)
    columns = jnp.arange(ep_count * capacity, dtype=jnp.int32)
    matches = target[:, :, None] == columns[None, None, :]
    placing = jnp.any(matches, axis=1).astype(jnp.bfloat16)
    weighting = jnp.sum(jnp.where(matches, route_weight[:, :, None], 0.0), axis=1)
    outgoing = lax.dot_general(
        placing, normed, (((0,), (0,)), ((), ())), preferred_element_type=jnp.float32
    ).astype(jnp.bfloat16)
    outgoing = outgoing.reshape(ep_count, capacity, model_width)
    arrived = lax.all_to_all(outgoing, "ep", split_axis=0, concat_axis=0, tiled=True)
    flat_rows = arrived.reshape(ep_count * capacity, model_width)
    activated = hidden_units(flat_rows, gate_up_weight, up_bias, tile)
    ones = jnp.full((ep_count * capacity, 128), 1.0 / 128, jnp.bfloat16)
    partial_value = project_down(
        activated, down_weight, lower_bias, ones, jnp.ones((1, 128), jnp.float32)
    )
    answered = lax.psum_scatter(partial_value, "tp", scatter_dimension=1, tiled=True)
    answered = answered.reshape(ep_count, capacity, quarter)
    came_back = lax.all_to_all(answered, "ep", split_axis=0, concat_axis=0, tiled=True)
    gathered = came_back.reshape(ep_count * capacity, quarter).astype(jnp.float32)
    layer_out = own_cols + jnp.dot(weighting, gathered, precision=lax.Precision.HIGHEST)
    return layer_out.astype(jnp.bfloat16)


def solution(mesh):
    placed = (
        P(("groups", "ep"), None),
        P(("groups", "ep"), None),
        P(("groups", "ep"), None),
        P(),
        P("ep", None, "tp"),
        P("ep", None, "tp"),
        P("ep", "tp"),
        P("ep", "tp", None),
        P("ep", "tp", None),
        P("ep", "tp"),
    )
    return jax.shard_map(
        shards, mesh=mesh, in_specs=placed, out_specs=P(("groups", "ep"), "tp"), check_vma=False
    )
```

```python
import jax
import jax.numpy as jnp
from jax import lax
from jax.experimental import pallas as pl
from jax.experimental.pallas import tpu as pltpu
from jax.sharding import PartitionSpec as P

VMEM_BYTES = 56 * 1024 * 1024
PIECES = 1
DOWN_TILE = 1536
HIDDEN_STEP = 512


def largest_step(total, limit, multiple):
    best = 0
    for size in range(multiple, min(total, limit) + 1, multiple):
        if total % size == 0:
            best = size
    return best or total


def decode_words(words, scale):
    word_count, width = words.shape
    shifts = lax.broadcasted_iota(jnp.int32, (1, 8, width), 1) * 4
    nibble = (words[:, None, :] >> shifts) & 15
    half = nibble.astype(jnp.float32).reshape(word_count * 8, width).astype(jnp.bfloat16) * 0.5
    negative = half >= 4.0
    magnit = jnp.where(negative, half - 4.0, half)
    value = magnit + jnp.maximum(magnit - 2.0, 0.0) + 2.0 * jnp.maximum(magnit - 3.0, 0.0)
    return value * jnp.where(negative, -scale, scale)


def gate_up_kernel(words_ref, scale_ref, bias_ref, out_ref, bias_out_ref, *, step, block_words):
    width = words_ref.shape[1]
    half = width // 2
    from_col = lax.broadcasted_iota(jnp.int32, (width, width), 0)
    to_col = lax.broadcasted_iota(jnp.int32, (width, width), 1)
    wanted = jnp.where(to_col < half, 2 * to_col, 2 * (to_col - half) + 1)
    parting = (from_col == wanted).astype(jnp.bfloat16)
    bias_out_ref[...] = jnp.dot(bias_ref[...], parting, preferred_element_type=jnp.float32)
    blocks = step // block_words
    scales = scale_ref[...].astype(jnp.float32)
    for part in range(words_ref.shape[0] // step):
        words = words_ref[part * step : (part + 1) * step, :]
        scale = scales[part * blocks : (part + 1) * blocks, :]
        spread = jnp.broadcast_to(scale[:, None, :], (blocks, block_words * 8, width))
        spread = spread.reshape(step * 8, width).astype(jnp.bfloat16)
        value = decode_words(words, spread)
        out_ref[part * step * 8 : (part + 1) * step * 8, :] = jnp.dot(
            value, parting, preferred_element_type=jnp.float32
        ).astype(jnp.bfloat16)


def unpack_gate_up(codes, scales, bias, tile):
    word_count, width = codes.shape
    block_words = word_count // scales.shape[0]
    step = largest_step(word_count, 80, 8)
    return pl.pallas_call(
        lambda *refs: gate_up_kernel(*refs, step=step, block_words=block_words),
        grid=(width // tile,),
        in_specs=[
            pl.BlockSpec((word_count, tile), lambda i: (0, i)),
            pl.BlockSpec((scales.shape[0], tile), lambda i: (0, i)),
            pl.BlockSpec((1, tile), lambda i: (0, i)),
        ],
        out_specs=[
            pl.BlockSpec((word_count * 8, tile), lambda i: (0, i)),
            pl.BlockSpec((1, tile), lambda i: (0, i)),
        ],
        out_shape=[
            jax.ShapeDtypeStruct((word_count * 8, width), jnp.bfloat16),
            jax.ShapeDtypeStruct((1, width), jnp.float32),
        ],
        compiler_params=pltpu.CompilerParams(vmem_limit_bytes=VMEM_BYTES),
        name="unpack_gate_up",
    )(codes, scales, bias)


def down_kernel(words_ref, scale_ref, out_ref):
    unit_count = words_ref.shape[1]
    block_count = scale_ref.shape[1]
    width = unit_count // block_count
    block_of = lax.broadcasted_iota(jnp.int32, (block_count, unit_count), 1) // width
    spreading = (block_of == lax.broadcasted_iota(jnp.int32, (block_count, unit_count), 0)).astype(
        jnp.bfloat16
    )
    spread = jnp.dot(scale_ref[...], spreading, preferred_element_type=jnp.float32)
    out_ref[...] = decode_words(words_ref[...], spread.astype(jnp.bfloat16))


def unpack_down(codes, scales):
    unit_count, word_count = codes.shape
    block_count = scales.shape[0]
    step = largest_step(word_count, 40, 8)
    return pl.pallas_call(
        down_kernel,
        grid=(word_count // step,),
        in_specs=[
            pl.BlockSpec((step, unit_count), lambda i: (i, 0)),
            pl.BlockSpec((step * 8, block_count), lambda i: (i, 0)),
        ],
        out_specs=pl.BlockSpec((step * 8, unit_count), lambda i: (i, 0)),
        out_shape=jax.ShapeDtypeStruct((word_count * 8, unit_count), jnp.bfloat16),
        compiler_params=pltpu.CompilerParams(vmem_limit_bytes=VMEM_BYTES),
        name="unpack_down",
    )(codes.T, scales.T)


def hidden_kernel(rows_ref, weight_ref, bias_ref, out_ref, *, tile):
    model_width, width = weight_ref.shape
    half = tile // 2
    for part in range(width // tile):
        columns = slice(part * tile, (part + 1) * tile)
        projected = jnp.dot(
            rows_ref[:, :model_width], weight_ref[:, columns], preferred_element_type=jnp.float32
        ) + bias_ref[:, columns]
        gate = jnp.minimum(projected[:, :half], 7.0)
        upward = jnp.clip(projected[:, half:], -7.0, 7.0)
        out_ref[:, part * half : (part + 1) * half] = (
            gate * jax.nn.sigmoid(1.702 * gate) * (upward + 1.0)
        ).astype(jnp.bfloat16)


def hidden_units(rows, weight, bias, tile):
    row_count = rows.shape[0]
    model_width, width = weight.shape
    step = largest_step(width, HIDDEN_STEP, tile)
    return pl.pallas_call(
        lambda *refs: hidden_kernel(*refs, tile=tile),
        grid=(width // step,),
        in_specs=[
            pl.BlockSpec(rows.shape, lambda i: (0, 0)),
            pl.BlockSpec((model_width, step), lambda i: (0, i)),
            pl.BlockSpec((1, step), lambda i: (0, i)),
        ],
        out_specs=pl.BlockSpec((row_count, step // 2), lambda i: (0, i)),
        out_shape=jax.ShapeDtypeStruct((row_count, width // 2), jnp.bfloat16),
        compiler_params=pltpu.CompilerParams(vmem_limit_bytes=VMEM_BYTES),
        name="hidden_units",
    )(rows, weight, bias)


def project_kernel(rows_ref, weight_ref, bias_ref, tail_ref, pick_ref, out_ref):
    value = lax.dot_general(
        rows_ref[...], weight_ref[...], (((1,), (1,)), ((), ())), preferred_element_type=jnp.float32
    )
    factor = jnp.sum(tail_ref[...].astype(jnp.float32) * pick_ref[...], axis=1, keepdims=True)
    out_ref[...] = ((value + bias_ref[...]) * factor).astype(jnp.bfloat16)


def project_down(rows, weight, bias, tail, pick):
    row_count, unit_count = rows.shape
    model_width = weight.shape[0]
    tile = DOWN_TILE
    return pl.pallas_call(
        project_kernel,
        grid=(pl.cdiv(model_width, tile),),
        in_specs=[
            pl.BlockSpec((row_count, unit_count), lambda i: (0, 0)),
            pl.BlockSpec((tile, unit_count), lambda i: (i, 0)),
            pl.BlockSpec((1, tile), lambda i: (0, i)),
            pl.BlockSpec((row_count, 128), lambda i: (0, tail.shape[1] // 128 - 1)),
            pl.BlockSpec((1, 128), lambda i: (0, 0)),
        ],
        out_specs=pl.BlockSpec((row_count, tile), lambda i: (0, i)),
        out_shape=jax.ShapeDtypeStruct((row_count, model_width), jnp.bfloat16),
        compiler_params=pltpu.CompilerParams(vmem_limit_bytes=VMEM_BYTES),
        name="project_down",
    )(rows, weight, bias, tail, pick)


def norm_kernel(hidden_ref, gain_ref, factor_ref, *out_refs, ep_count):
    tok_count, model_width = hidden_ref.shape
    total = out_refs[0].shape[1]
    widened = hidden_ref[...].astype(jnp.float32)
    mean_square = jnp.mean(widened * widened, axis=-1, keepdims=True)
    normed = (widened * lax.rsqrt(mean_square + 1e-05) * gain_ref[...].astype(jnp.float32)).astype(
        jnp.bfloat16
    )
    tail = total - model_width
    place = lax.broadcasted_iota(jnp.int32, (tok_count, tail), 1) - (tail - 3 * ep_count)
    factor = factor_ref[...]
    upper = factor.astype(jnp.bfloat16).astype(jnp.float32)
    rest = factor - upper
    middle = rest.astype(jnp.bfloat16).astype(jnp.float32)
    pieces = jnp.where(place < ep_count, upper, jnp.where(place < 2 * ep_count, middle, rest - middle))
    pieces = pieces.astype(jnp.bfloat16)
    step = tok_count // len(out_refs)
    for i, out_ref in enumerate(out_refs):
        out_ref[:, :model_width] = normed[i * step : (i + 1) * step]
        out_ref[:, model_width:] = pieces[i * step : (i + 1) * step]


def normed_with_factors(hidden, gain, route_experts, route_weight, ep_count, pieces):
    tok_count, model_width = hidden.shape
    total = -(-(model_width + 3 * ep_count) // 128) * 128
    shape = jax.ShapeDtypeStruct((tok_count // pieces, total), jnp.bfloat16)
    place = jnp.arange(total - model_width, dtype=jnp.int32) - (total - model_width - 3 * ep_count)
    expert = jnp.where(place < 0, -1, place % ep_count)
    factor = jnp.sum(
        jnp.where(route_experts[:, :, None] == expert, route_weight[:, :, None], 0.0), axis=1
    )
    return pl.pallas_call(
        lambda *refs: norm_kernel(*refs, ep_count=ep_count),
        out_shape=[shape] * pieces,
        compiler_params=pltpu.CompilerParams(vmem_limit_bytes=VMEM_BYTES),
        name="norm",
    )(hidden, gain.astype(jnp.float32).reshape(1, -1), factor)


def rms_normed(hidden, norm_gain):
    widened = hidden.astype(jnp.float32)
    mean_square = jnp.mean(widened * widened, axis=-1, keepdims=True)
    scaled = widened * lax.rsqrt(mean_square + 1e-05) * norm_gain.astype(jnp.float32)
    return scaled.astype(jnp.bfloat16)


def tp_sum(rows, tp_rank, tp_count, quarter):
    summed = lax.dynamic_slice_in_dim(rows, tp_rank * quarter, quarter, 1).astype(jnp.float32)
    for away in range(1, tp_count):
        other = (tp_rank + away) % tp_count
        sent = lax.dynamic_slice_in_dim(rows, other * quarter, quarter, 1)
        got = lax.ppermute(sent, "tp", [(k, (k + away) % tp_count) for k in range(tp_count)])
        summed = summed + got.astype(jnp.float32)
    return summed


def shards(
    hidden,
    route_experts,
    route_weight,
    norm_gain,
    gate_up_codes,
    gate_up_scales,
    gate_up_bias,
    down_codes,
    down_scales,
    down_bias,
):
    ep_count = lax.axis_size("ep")
    ep_rank = lax.axis_index("ep")
    tp_count = lax.axis_size("tp")
    tp_rank = lax.axis_index("tp")
    tok_count, model_width = hidden.shape
    top_count = route_experts.shape[1]
    quarter = model_width // tp_count
    tile = 256
    capacity = min(tok_count, max(tp_count, 2 * tok_count * top_count // ep_count))
    gate_up_weight, up_bias = unpack_gate_up(
        gate_up_codes[0], gate_up_scales[0], gate_up_bias, tile
    )
    down_weight = unpack_down(down_codes[0], down_scales[0])
    own_cols = lax.dynamic_slice_in_dim(hidden, tp_rank * quarter, quarter, 1).astype(jnp.float32)
    own_bias = down_bias.astype(jnp.float32)
    lower_bias = lax.dynamic_update_slice(
        jnp.zeros((1, model_width), jnp.float32), own_bias, (0, tp_rank * quarter)
    )

    if capacity == tok_count and 3 * ep_count <= 128:
        place = jnp.arange(128, dtype=jnp.int32) - (128 - 3 * ep_count)
        pick = ((place >= 0) & (place % ep_count == ep_rank)).astype(jnp.float32).reshape(1, 128)
        outgoing = normed_with_factors(
            hidden, norm_gain, route_experts, route_weight, ep_count, PIECES
        )
        arrived = [lax.all_gather(rows, "ep", axis=0, tiled=True) for rows in outgoing]
        outputs = []
        for rows in arrived:
            activated = hidden_units(rows, gate_up_weight, up_bias, tile)
            answered = project_down(activated, down_weight, lower_bias, rows, pick)
            summed = lax.psum_scatter(answered, "ep", scatter_dimension=0, tiled=True)
            outputs.append(tp_sum(summed, tp_rank, tp_count, quarter))
        summed = outputs[0] if PIECES == 1 else jnp.concatenate(outputs, axis=0)
        return (own_cols + summed).astype(jnp.bfloat16)

    normed = rms_normed(hidden, norm_gain)
    flat_routes = route_experts.reshape(-1)
    onehot = (flat_routes[:, None] == jnp.arange(ep_count, dtype=jnp.int32)[None, :]).astype(
        jnp.int32
    )
    before = jnp.cumsum(onehot, axis=0) - onehot
    slot_of = jnp.sum(before * onehot, axis=1)
    target = (flat_routes * capacity + slot_of).reshape(tok_count, top_count)
    columns = jnp.arange(ep_count * capacity, dtype=jnp.int32)
    matches = target[:, :, None] == columns[None, None, :]
    placing = jnp.any(matches, axis=1).astype(jnp.bfloat16)
    weighting = jnp.sum(jnp.where(matches, route_weight[:, :, None], 0.0), axis=1)
    outgoing = lax.dot_general(
        placing, normed, (((0,), (0,)), ((), ())), preferred_element_type=jnp.float32
    ).astype(jnp.bfloat16)
    outgoing = outgoing.reshape(ep_count, capacity, model_width)
    arrived = lax.all_to_all(outgoing, "ep", split_axis=0, concat_axis=0, tiled=True)
    flat_rows = arrived.reshape(ep_count * capacity, model_width)
    activated = hidden_units(flat_rows, gate_up_weight, up_bias, tile)
    ones = jnp.full((ep_count * capacity, 128), 1.0 / 128, jnp.bfloat16)
    partial_value = project_down(
        activated, down_weight, lower_bias, ones, jnp.ones((1, 128), jnp.float32)
    )
    answered = lax.psum_scatter(partial_value, "tp", scatter_dimension=1, tiled=True)
    answered = answered.reshape(ep_count, capacity, quarter)
    came_back = lax.all_to_all(answered, "ep", split_axis=0, concat_axis=0, tiled=True)
    gathered = came_back.reshape(ep_count * capacity, quarter).astype(jnp.float32)
    layer_out = own_cols + jnp.dot(weighting, gathered, precision=lax.Precision.HIGHEST)
    return layer_out.astype(jnp.bfloat16)


def solution(mesh):
    placed = (
        P(("groups", "ep"), None),
        P(("groups", "ep"), None),
        P(("groups", "ep"), None),
        P(),
        P("ep", None, "tp"),
        P("ep", None, "tp"),
        P("ep", "tp"),
        P("ep", "tp", None),
        P("ep", "tp", None),
        P("ep", "tp"),
    )
    return jax.shard_map(
        shards, mesh=mesh, in_specs=placed, out_specs=P(("groups", "ep"), "tp"), check_vma=False
    )
```

```python
import jax
import jax.numpy as jnp
from jax import lax
from jax.experimental import pallas as pl
from jax.experimental.pallas import tpu as pltpu
from jax.sharding import PartitionSpec as P

VMEM_BYTES = 56 * 1024 * 1024
PIECES = 1
DOWN_TILE = 1536
HIDDEN_STEP = 512


def largest_step(total, limit, multiple):
    best = 0
    for size in range(multiple, min(total, limit) + 1, multiple):
        if total % size == 0:
            best = size
    return best or total


def decode_words(words, scale):
    word_count, width = words.shape
    shifts = lax.broadcasted_iota(jnp.int32, (1, 8, width), 1) * 4
    nibble = (words[:, None, :] >> shifts) & 15
    half = nibble.astype(jnp.float32).reshape(word_count * 8, width).astype(jnp.bfloat16) * 0.5
    negative = half >= 4.0
    magnit = jnp.where(negative, half - 4.0, half)
    value = magnit + jnp.maximum(magnit - 2.0, 0.0) + 2.0 * jnp.maximum(magnit - 3.0, 0.0)
    return value * jnp.where(negative, -scale, scale)


def gate_up_kernel(words_ref, scale_ref, bias_ref, out_ref, bias_out_ref, *, step, block_words):
    width = words_ref.shape[1]
    half = width // 2
    from_col = lax.broadcasted_iota(jnp.int32, (width, width), 0)
    to_col = lax.broadcasted_iota(jnp.int32, (width, width), 1)
    wanted = jnp.where(to_col < half, 2 * to_col, 2 * (to_col - half) + 1)
    parting = (from_col == wanted).astype(jnp.bfloat16)
    bias_out_ref[...] = jnp.dot(bias_ref[...], parting, preferred_element_type=jnp.float32)
    blocks = step // block_words
    scales = scale_ref[...].astype(jnp.float32)
    for part in range(words_ref.shape[0] // step):
        words = words_ref[part * step : (part + 1) * step, :]
        scale = scales[part * blocks : (part + 1) * blocks, :]
        spread = jnp.broadcast_to(scale[:, None, :], (blocks, block_words * 8, width))
        spread = spread.reshape(step * 8, width).astype(jnp.bfloat16)
        value = decode_words(words, spread)
        out_ref[part * step * 8 : (part + 1) * step * 8, :] = jnp.dot(
            value, parting, preferred_element_type=jnp.float32
        ).astype(jnp.bfloat16)


def unpack_gate_up(codes, scales, bias, tile):
    word_count, width = codes.shape
    block_words = word_count // scales.shape[0]
    step = largest_step(word_count, 80, 8)
    return pl.pallas_call(
        lambda *refs: gate_up_kernel(*refs, step=step, block_words=block_words),
        grid=(width // tile,),
        in_specs=[
            pl.BlockSpec((word_count, tile), lambda i: (0, i)),
            pl.BlockSpec((scales.shape[0], tile), lambda i: (0, i)),
            pl.BlockSpec((1, tile), lambda i: (0, i)),
        ],
        out_specs=[
            pl.BlockSpec((word_count * 8, tile), lambda i: (0, i)),
            pl.BlockSpec((1, tile), lambda i: (0, i)),
        ],
        out_shape=[
            jax.ShapeDtypeStruct((word_count * 8, width), jnp.bfloat16),
            jax.ShapeDtypeStruct((1, width), jnp.float32),
        ],
        compiler_params=pltpu.CompilerParams(vmem_limit_bytes=VMEM_BYTES),
        name="unpack_gate_up",
    )(codes, scales, bias)


def down_kernel(words_ref, scale_ref, out_ref):
    unit_count = words_ref.shape[1]
    block_count = scale_ref.shape[1]
    width = unit_count // block_count
    block_of = lax.broadcasted_iota(jnp.int32, (block_count, unit_count), 1) // width
    spreading = (block_of == lax.broadcasted_iota(jnp.int32, (block_count, unit_count), 0)).astype(
        jnp.bfloat16
    )
    spread = jnp.dot(scale_ref[...], spreading, preferred_element_type=jnp.float32)
    out_ref[...] = decode_words(words_ref[...], spread.astype(jnp.bfloat16))


def unpack_down(codes, scales):
    unit_count, word_count = codes.shape
    block_count = scales.shape[0]
    step = largest_step(word_count, 40, 8)
    return pl.pallas_call(
        down_kernel,
        grid=(word_count // step,),
        in_specs=[
            pl.BlockSpec((step, unit_count), lambda i: (i, 0)),
            pl.BlockSpec((step * 8, block_count), lambda i: (i, 0)),
        ],
        out_specs=pl.BlockSpec((step * 8, unit_count), lambda i: (i, 0)),
        out_shape=jax.ShapeDtypeStruct((word_count * 8, unit_count), jnp.bfloat16),
        compiler_params=pltpu.CompilerParams(vmem_limit_bytes=VMEM_BYTES),
        name="unpack_down",
    )(codes.T, scales.T)


def hidden_kernel(rows_ref, weight_ref, bias_ref, out_ref, *, tile):
    model_width, width = weight_ref.shape
    half = tile // 2
    for part in range(width // tile):
        columns = slice(part * tile, (part + 1) * tile)
        projected = jnp.dot(
            rows_ref[:, :model_width], weight_ref[:, columns], preferred_element_type=jnp.float32
        ) + bias_ref[:, columns]
        gate = jnp.minimum(projected[:, :half], 7.0)
        upward = jnp.clip(projected[:, half:], -7.0, 7.0)
        out_ref[:, part * half : (part + 1) * half] = (
            gate * jax.nn.sigmoid(1.702 * gate) * (upward + 1.0)
        ).astype(jnp.bfloat16)


def hidden_units(rows, weight, bias, tile):
    row_count = rows.shape[0]
    model_width, width = weight.shape
    step = largest_step(width, HIDDEN_STEP, tile)
    return pl.pallas_call(
        lambda *refs: hidden_kernel(*refs, tile=tile),
        grid=(width // step,),
        in_specs=[
            pl.BlockSpec(rows.shape, lambda i: (0, 0)),
            pl.BlockSpec((model_width, step), lambda i: (0, i)),
            pl.BlockSpec((1, step), lambda i: (0, i)),
        ],
        out_specs=pl.BlockSpec((row_count, step // 2), lambda i: (0, i)),
        out_shape=jax.ShapeDtypeStruct((row_count, width // 2), jnp.bfloat16),
        compiler_params=pltpu.CompilerParams(vmem_limit_bytes=VMEM_BYTES),
        name="hidden_units",
    )(rows, weight, bias)


def project_kernel(rows_ref, weight_ref, bias_ref, tail_ref, pick_ref, out_ref):
    value = lax.dot_general(
        rows_ref[...], weight_ref[...], (((1,), (1,)), ((), ())), preferred_element_type=jnp.float32
    )
    factor = jnp.sum(tail_ref[...].astype(jnp.float32) * pick_ref[...], axis=1, keepdims=True)
    out_ref[...] = ((value + bias_ref[...]) * factor).astype(jnp.bfloat16)


def project_down(rows, weight, bias, tail, pick):
    row_count, unit_count = rows.shape
    model_width = weight.shape[0]
    tile = DOWN_TILE
    return pl.pallas_call(
        project_kernel,
        grid=(pl.cdiv(model_width, tile),),
        in_specs=[
            pl.BlockSpec((row_count, unit_count), lambda i: (0, 0)),
            pl.BlockSpec((tile, unit_count), lambda i: (i, 0)),
            pl.BlockSpec((1, tile), lambda i: (0, i)),
            pl.BlockSpec((row_count, 128), lambda i: (0, tail.shape[1] // 128 - 1)),
            pl.BlockSpec((1, 128), lambda i: (0, 0)),
        ],
        out_specs=pl.BlockSpec((row_count, tile), lambda i: (0, i)),
        out_shape=jax.ShapeDtypeStruct((row_count, model_width), jnp.bfloat16),
        compiler_params=pltpu.CompilerParams(vmem_limit_bytes=VMEM_BYTES),
        name="project_down",
    )(rows, weight, bias, tail, pick)


def norm_kernel(hidden_ref, gain_ref, factor_ref, *out_refs, ep_count):
    tok_count, model_width = hidden_ref.shape
    total = out_refs[0].shape[1]
    widened = hidden_ref[...].astype(jnp.float32)
    mean_square = jnp.mean(widened * widened, axis=-1, keepdims=True)
    normed = (widened * lax.rsqrt(mean_square + 1e-05) * gain_ref[...].astype(jnp.float32)[None, :]).astype(
        jnp.bfloat16
    )
    tail = total - model_width
    place = lax.broadcasted_iota(jnp.int32, (tok_count, tail), 1) - (tail - 3 * ep_count)
    factor = factor_ref[...]
    upper = factor.astype(jnp.bfloat16).astype(jnp.float32)
    rest = factor - upper
    middle = rest.astype(jnp.bfloat16).astype(jnp.float32)
    pieces = jnp.where(place < ep_count, upper, jnp.where(place < 2 * ep_count, middle, rest - middle))
    pieces = pieces.astype(jnp.bfloat16)
    step = tok_count // len(out_refs)
    for i, out_ref in enumerate(out_refs):
        out_ref[:, :model_width] = normed[i * step : (i + 1) * step]
        out_ref[:, model_width:] = pieces[i * step : (i + 1) * step]


def normed_with_factors(hidden, gain, route_experts, route_weight, ep_count, pieces):
    tok_count, model_width = hidden.shape
    total = -(-(model_width + 3 * ep_count) // 128) * 128
    shape = jax.ShapeDtypeStruct((tok_count // pieces, total), jnp.bfloat16)
    place = jnp.arange(total - model_width, dtype=jnp.int32) - (total - model_width - 3 * ep_count)
    expert = jnp.where(place < 0, -1, place % ep_count)
    factor = jnp.sum(
        jnp.where(route_experts[:, :, None] == expert, route_weight[:, :, None], 0.0), axis=1
    )
    return pl.pallas_call(
        lambda *refs: norm_kernel(*refs, ep_count=ep_count),
        out_shape=[shape] * pieces,
        compiler_params=pltpu.CompilerParams(vmem_limit_bytes=VMEM_BYTES),
        name="norm",
    )(hidden, gain, factor)


def rms_normed(hidden, norm_gain):
    widened = hidden.astype(jnp.float32)
    mean_square = jnp.mean(widened * widened, axis=-1, keepdims=True)
    scaled = widened * lax.rsqrt(mean_square + 1e-05) * norm_gain.astype(jnp.float32)
    return scaled.astype(jnp.bfloat16)


def tp_sum(rows, tp_rank, tp_count, quarter):
    summed = lax.dynamic_slice_in_dim(rows, tp_rank * quarter, quarter, 1).astype(jnp.float32)
    for away in range(1, tp_count):
        other = (tp_rank + away) % tp_count
        sent = lax.dynamic_slice_in_dim(rows, other * quarter, quarter, 1)
        got = lax.ppermute(sent, "tp", [(k, (k + away) % tp_count) for k in range(tp_count)])
        summed = summed + got.astype(jnp.float32)
    return summed


def shards(
    hidden,
    route_experts,
    route_weight,
    norm_gain,
    gate_up_codes,
    gate_up_scales,
    gate_up_bias,
    down_codes,
    down_scales,
    down_bias,
):
    ep_count = lax.axis_size("ep")
    ep_rank = lax.axis_index("ep")
    tp_count = lax.axis_size("tp")
    tp_rank = lax.axis_index("tp")
    tok_count, model_width = hidden.shape
    top_count = route_experts.shape[1]
    quarter = model_width // tp_count
    tile = 256
    capacity = min(tok_count, max(tp_count, 2 * tok_count * top_count // ep_count))
    gate_up_weight, up_bias = unpack_gate_up(
        gate_up_codes[0], gate_up_scales[0], gate_up_bias, tile
    )
    down_weight = unpack_down(down_codes[0], down_scales[0])
    own_cols = lax.dynamic_slice_in_dim(hidden, tp_rank * quarter, quarter, 1).astype(jnp.float32)
    own_bias = down_bias.astype(jnp.float32)
    lower_bias = lax.dynamic_update_slice(
        jnp.zeros((1, model_width), jnp.float32), own_bias, (0, tp_rank * quarter)
    )

    if capacity == tok_count and 3 * ep_count <= 128:
        place = jnp.arange(128, dtype=jnp.int32) - (128 - 3 * ep_count)
        pick = ((place >= 0) & (place % ep_count == ep_rank)).astype(jnp.float32).reshape(1, 128)
        outgoing = normed_with_factors(
            hidden, norm_gain, route_experts, route_weight, ep_count, PIECES
        )
        arrived = [lax.all_gather(rows, "ep", axis=0, tiled=True) for rows in outgoing]
        outputs = []
        for rows in arrived:
            activated = hidden_units(rows, gate_up_weight, up_bias, tile)
            answered = project_down(activated, down_weight, lower_bias, rows, pick)
            summed = lax.psum_scatter(answered, "ep", scatter_dimension=0, tiled=True)
            outputs.append(tp_sum(summed, tp_rank, tp_count, quarter))
        summed = outputs[0] if PIECES == 1 else jnp.concatenate(outputs, axis=0)
        return (own_cols + summed).astype(jnp.bfloat16)

    normed = rms_normed(hidden, norm_gain)
    flat_routes = route_experts.reshape(-1)
    onehot = (flat_routes[:, None] == jnp.arange(ep_count, dtype=jnp.int32)[None, :]).astype(
        jnp.int32
    )
    before = jnp.cumsum(onehot, axis=0) - onehot
    slot_of = jnp.sum(before * onehot, axis=1)
    target = (flat_routes * capacity + slot_of).reshape(tok_count, top_count)
    columns = jnp.arange(ep_count * capacity, dtype=jnp.int32)
    matches = target[:, :, None] == columns[None, None, :]
    placing = jnp.any(matches, axis=1).astype(jnp.bfloat16)
    weighting = jnp.sum(jnp.where(matches, route_weight[:, :, None], 0.0), axis=1)
    outgoing = lax.dot_general(
        placing, normed, (((0,), (0,)), ((), ())), preferred_element_type=jnp.float32
    ).astype(jnp.bfloat16)
    outgoing = outgoing.reshape(ep_count, capacity, model_width)
    arrived = lax.all_to_all(outgoing, "ep", split_axis=0, concat_axis=0, tiled=True)
    flat_rows = arrived.reshape(ep_count * capacity, model_width)
    activated = hidden_units(flat_rows, gate_up_weight, up_bias, tile)
    ones = jnp.full((ep_count * capacity, 128), 1.0 / 128, jnp.bfloat16)
    partial_value = project_down(
        activated, down_weight, lower_bias, ones, jnp.ones((1, 128), jnp.float32)
    )
    answered = lax.psum_scatter(partial_value, "tp", scatter_dimension=1, tiled=True)
    answered = answered.reshape(ep_count, capacity, quarter)
    came_back = lax.all_to_all(answered, "ep", split_axis=0, concat_axis=0, tiled=True)
    gathered = came_back.reshape(ep_count * capacity, quarter).astype(jnp.float32)
    layer_out = own_cols + jnp.dot(weighting, gathered, precision=lax.Precision.HIGHEST)
    return layer_out.astype(jnp.bfloat16)


def solution(mesh):
    placed = (
        P(("groups", "ep"), None),
        P(("groups", "ep"), None),
        P(("groups", "ep"), None),
        P(),
        P("ep", None, "tp"),
        P("ep", None, "tp"),
        P("ep", "tp"),
        P("ep", "tp", None),
        P("ep", "tp", None),
        P("ep", "tp"),
    )
    return jax.shard_map(
        shards, mesh=mesh, in_specs=placed, out_specs=P(("groups", "ep"), "tp"), check_vma=False
    )
```
